16 devices in a mesh: dp: 4 (over y, z), tp: 4 (over x, core).
Axes of the slice: x: 2, y: 2, z: 2, core: 2. Of those that a mesh axis runs over, the one named last changes fastest.
Arguments:
- x: bfloat16 [4, 2048, 2048], P('dp', 'tp')
- dy: bfloat16 [4, 2048, 2048], P('dp', 'tp')
- wq: bfloat16 [2048, 3072], P('dp', 'tp')
- wk: bfloat16 [2048, 512], P('dp', 'tp')
- wv: bfloat16 [2048, 512], P('dp', 'tp')
- wo: bfloat16 [3072, 2048], P(('tp', 'dp'))
- w_gate: bfloat16 [2048, 8192], P('dp', 'tp')
- w_up: bfloat16 [2048, 8192], P('dp', 'tp')
- w_down: bfloat16 [8192, 2048], P(('tp', 'dp'))
Outputs:
- output 1: bfloat16 [4, 2048, 2048], P('dp', 'tp')
- output 2: bfloat16 [2048, 3072], P('dp', 'tp')
- output 3: bfloat16 [2048, 512], P('dp', 'tp')
- output 4: bfloat16 [2048, 512], P('dp', 'tp')
- output 5: bfloat16 [3072, 2048], P(('tp', 'dp'))
- output 6: bfloat16 [2048, 8192], P('dp', 'tp')
- output 7: bfloat16 [2048, 8192], P('dp', 'tp')
- output 8: bfloat16 [8192, 2048], P(('tp', 'dp'))
All inputs are finite; a program needn't handle non-finite values.
Results may differ from the reference program's by a relative error of at most 0.024.
Values are sent between devices in bfloat16 or wider.
A program may use at most 2 GiB of HBM per device.

```python
import jax
import jax.numpy as jnp
from jax import lax

SEQUENCES = 4
TOKENS = 2048
D = 2048
HEADS = 24
KV_HEADS = 4
HEAD = 128
FF = 8192
THETA = 10000
NAMES = ("wq", "wk", "wv", "wo", "w_gate", "w_up", "w_down")
SHAPES = {
    "wq": (D, HEADS * HEAD),
    "wk": (D, KV_HEADS * HEAD),
    "wv": (D, KV_HEADS * HEAD),
    "wo": (HEADS * HEAD, D),
    "w_gate": (D, FF),
    "w_up": (D, FF),
    "w_down": (FF, D),
}


def bump(key, n, height):
    away = (jnp.arange(n, dtype=jnp.int32) - jax.random.randint(key, (), 0, n, jnp.int32)) % n
    return jnp.where(away < n // 8, height, 1.0)


def together(key, own, strength):
    shared = jax.random.normal(key, own.shape[1:], jnp.float32)
    return (own + strength * shared) * lax.rsqrt(1 + strength * strength)


def setup_inputs(seed: int = 0, part: int = 0) -> dict:
    kx, kdy, ka, kb, kz, kf, kh, kl, *kw = jax.random.split(jax.random.key(seed), 8 + len(NAMES))
    shape = (SEQUENCES, TOKENS, D)
    much_x, much_dy = jax.random.uniform(kz, (2,), jnp.float32, 0.0, 1.0)
    loud = 2.0 ** jax.random.uniform(jax.random.fold_in(kz, 1), (), jnp.float32, -1.0, 2.0)
    halves = 2.0 ** jax.random.uniform(kl, (2,), jnp.float32, -1.0, 1.0)
    times = {"wq": 1.0, "wk": 1.0, "wv": 2.0, "wo": halves[0], "w_gate": 1.0, "w_up": bump(kh, FF, 4.0), "w_down": halves[1]}
    x = together(ka, jax.random.normal(kx, shape, jnp.float32), much_x) * bump(kf, D, 4.0)
    dy = together(kb, jax.random.normal(kdy, shape, jnp.float32), much_dy)
    drawn = {"x": x.astype(jnp.bfloat16), "dy": (loud * dy * (SEQUENCES * TOKENS) ** -0.5).astype(jnp.bfloat16)}
    for key, name in zip(kw, NAMES, strict=True):
        drawn[name] = (jax.random.normal(key, SHAPES[name], jnp.float32) * SHAPES[name][0] ** -0.5 * times[name]).astype(jnp.bfloat16)
    return drawn


def matmul(a, w):
    return jnp.dot(a, w, preferred_element_type=jnp.float32).astype(jnp.bfloat16)


def normed(h):
    wide = h.astype(jnp.float32)
    scale = lax.rsqrt(jnp.mean(wide**2, -1, keepdims=True) + 1e-6)
    return (wide * scale).astype(jnp.bfloat16)


def turned(t, theta):
    half = t.shape[-1] // 2
    angle = jnp.arange(t.shape[0], dtype=jnp.float32)[:, None] * theta ** (-jnp.arange(half, dtype=jnp.float32) / half)
    cos, sin = jnp.cos(angle)[:, None], jnp.sin(angle)[:, None]
    a, b = t[..., :half].astype(jnp.float32), t[..., half:].astype(jnp.float32)
    return jnp.concatenate([a * cos - b * sin, b * cos + a * sin], -1).astype(jnp.bfloat16)


def seen_by(q, k, v):
    tokens, kv = q.shape[0], k.shape[1]
    q = q.reshape(tokens, kv, -1, q.shape[-1])
    scores = jnp.einsum("tgsd,ugd->gstu", q.astype(jnp.float32), k.astype(jnp.float32)) * q.shape[-1] ** -0.5
    place = jnp.arange(tokens)
    weights = jax.nn.softmax(jnp.where(place[:, None] >= place, scores, -jnp.inf), -1).astype(jnp.bfloat16)
    return jnp.einsum("gstu,ugd->tgsd", weights.astype(jnp.float32), v.astype(jnp.float32)).astype(jnp.bfloat16).reshape(tokens, -1)


def layer(h, w):
    a = normed(h)
    q, k = (turned(matmul(a, w[name]).reshape(h.shape[0], -1, HEAD), THETA) for name in ("wq", "wk"))
    h = h + matmul(seen_by(q, k, matmul(a, w["wv"]).reshape(h.shape[0], -1, HEAD)), w["wo"])
    b = normed(h)
    gate = jnp.dot(b, w["w_gate"], preferred_element_type=jnp.float32)
    up = jnp.dot(b, w["w_up"], preferred_element_type=jnp.float32)
    return h + matmul((jax.nn.silu(gate) * up).astype(jnp.bfloat16), w["w_down"])


def reference(x, dy, wq, wk, wv, wo, w_gate, w_up, w_down):
    weights = dict(zip(NAMES, (wq, wk, wv, wo, w_gate, w_up, w_down), strict=True))

    def take(so_far, sequence):
        h, by_y = sequence
        _, back = jax.vjp(lambda w, h: layer(h, w), weights, h)
        by_weights, by_h = back(by_y)
        return jax.tree.map(lambda total, term: total + term.astype(jnp.float32), so_far, by_weights), by_h

    none_yet = {name: jnp.zeros(w.shape, jnp.float32) for name, w in weights.items()}
    by_weights, by_x = lax.scan(take, none_yet, (x, dy))
    return (by_x, *(by_weights[name].astype(jnp.bfloat16) for name in NAMES))
```

```python
import functools

import jax
import jax.numpy as jnp
from jax import lax
from jax.experimental import pallas as pl
from jax.experimental.pallas import tpu as pltpu
from jax.sharding import PartitionSpec as P


HEAD = 128
THETA = 10000
NEG = -1e30
HIDDEN = 2 * NEG
LOG2E = 1.4426950408889634
VMEM = 56 * 2**20
BLOCK = 512
f32, bf16 = jnp.float32, jnp.bfloat16


def _dot(a, b, ca, cb):
    return lax.dot_general(a, b, (((ca,), (cb,)), ((), ())), preferred_element_type=f32)


def _turn(t, cos, sin):
    return t * cos + pltpu.roll(t, HEAD // 2, 1) * sin


def _attn_fwd(me_ref, q_ref, k_ref, v_ref, cos_ref, sin_ref, o_ref, lse_ref, k_s, q_s, top_s, mix_s, *, heads, blocks, scale):
    me, iq = me_ref[0], pl.program_id(0)
    e = scale * LOG2E
    n = BLOCK

    @pl.when(iq == 0)
    def _():
        for j in range(blocks):
            rows = pl.ds(pl.multiple_of((j ^ me) * n, n), n)
            here = slice(j * n, (j + 1) * n)
            k_s[here, :] = _turn(k_ref[rows, :].astype(f32), cos_ref[here, :], sin_ref[here, :]).astype(bf16)

    mine = pl.ds(pl.multiple_of(iq * n, n), n)
    cos, sin = cos_ref[mine, :], sin_ref[mine, :]
    for h in range(heads):
        q_s[h] = _turn(q_ref[:, h * HEAD : (h + 1) * HEAD].astype(f32), cos, sin).astype(bf16)
    top_s[...] = jnp.full(top_s.shape, NEG, f32)
    mix_s[...] = jnp.zeros(mix_s.shape, f32)
    ones = jnp.ones((8, n), bf16)

    def block(j, masked):
        here = pl.ds(pl.multiple_of(j * n, n), n)
        rows = pl.ds(pl.multiple_of((j ^ me) * n, n), n)
        k = k_s[here, :]
        scores = [_dot(k, q_s[h], 1, 1) for h in range(heads)]
        if masked:
            ok = lax.broadcasted_iota(jnp.int32, (n, n), 1) >= lax.broadcasted_iota(jnp.int32, (n, n), 0)
        weights, keeps = [], []
        for h, s in enumerate(scores):
            if masked:
                s = jnp.where(ok, s, HIDDEN)
            old = top_s[h : h + 1, :]
            top = jnp.maximum(old, s.max(axis=0, keepdims=True))
            top_s[h : h + 1, :] = top
            weights.append(jnp.exp2((s - top) * e).astype(bf16))
            keeps.append(jnp.exp2((old - top) * e))
        values = jnp.concatenate([v_ref[rows, :].T, ones], axis=0)
        for h in range(heads):
            mix_s[h] = mix_s[h] * keeps[h] + _dot(values, weights[h], 1, 0)

    lax.fori_loop(0, iq, lambda j, _: block(j, False), None)
    block(iq, True)
    for h in range(heads):
        total = mix_s[h, HEAD : HEAD + 1, :]
        o_ref[:, h * HEAD : (h + 1) * HEAD] = (mix_s[h, :HEAD, :] * (1 / total)).T.astype(bf16)
        lse_ref[h : h + 1, :] = top_s[h : h + 1, :] * scale + jnp.log(total)


def _attn_bwd(me_ref, q_ref, k_ref, v_ref, cos_ref, sin_ref, o_ref, do_ref, lse_ref, d_ref, k_s, q_s, stat_s, dq_s, dk_s, dv_s, *, heads, blocks, scale):
    me, iq = me_ref[0], pl.program_id(0)
    e = scale * LOG2E
    n = BLOCK

    @pl.when(iq == 0)
    def _():
        for j in range(blocks):
            rows = pl.ds(pl.multiple_of((j ^ me) * n, n), n)
            here = slice(j * n, (j + 1) * n)
            k_s[here, :] = _turn(k_ref[rows, :].astype(f32), cos_ref[here, :], sin_ref[here, :]).astype(bf16)
        dk_s[...] = jnp.zeros_like(dk_s)
        dv_s[...] = jnp.zeros_like(dv_s)

    mine = pl.ds(pl.multiple_of(iq * n, n), n)
    cos, sin = cos_ref[mine, :], sin_ref[mine, :]
    for h in range(heads):
        cols = slice(h * HEAD, (h + 1) * HEAD)
        q_s[h] = _turn(q_ref[:, cols].astype(f32), cos, sin).astype(bf16)
        both = (do_ref[:, cols].astype(f32) * o_ref[:, cols].astype(f32)).T
        stat_s[h : h + 1, :] = both.sum(axis=0, keepdims=True)
    dq_s[...] = jnp.zeros_like(dq_s)

    def block(j, masked):
        here = pl.ds(pl.multiple_of(j * n, n), n)
        rows = pl.ds(pl.multiple_of((j ^ me) * n, n), n)
        k, v = k_s[here, :], v_ref[rows, :]
        dos = [do_ref[:, h * HEAD : (h + 1) * HEAD] for h in range(heads)]
        scores = [_dot(k, q_s[h], 1, 1) for h in range(heads)]
        dps = [_dot(v, dos[h], 1, 1) for h in range(heads)]
        kt = k.T
        if masked:
            ok = lax.broadcasted_iota(jnp.int32, (n, n), 1) >= lax.broadcasted_iota(jnp.int32, (n, n), 0)
        for h in range(heads):
            p = jnp.exp2(scores[h] * e - lse_ref[h : h + 1, :] * LOG2E)
            if masked:
                p = jnp.where(ok, p, 0.0)
            ds = (p * (dps[h] - stat_s[h : h + 1, :])).astype(bf16)
            dv_s[here, :] += _dot(p.astype(bf16), dos[h], 1, 0)
            dk_s[here, :] += _dot(ds, q_s[h], 1, 0)
            dq_s[h] += _dot(kt, ds, 1, 0)

    lax.fori_loop(0, iq, lambda j, _: block(j, False), None)
    block(iq, True)
    place = pl.ds(pl.multiple_of((iq ^ me) * n, n), n)
    for h in range(heads):
        d_ref[place, h * HEAD : (h + 1) * HEAD] = _turn((dq_s[h] * scale).T, cos, -sin).astype(bf16)

    @pl.when(iq == blocks - 1)
    def _():
        at = heads * HEAD
        for j in range(blocks):
            rows = pl.ds(pl.multiple_of((j ^ me) * n, n), n)
            here = slice(j * n, (j + 1) * n)
            d_ref[rows, at : at + HEAD] = _turn(dk_s[here, :] * scale, cos_ref[here, :], -sin_ref[here, :]).astype(bf16)
            d_ref[rows, at + HEAD : at + 2 * HEAD] = dv_s[here, :].astype(bf16)


def _attn_specs(tokens, heads):
    wide = heads * HEAD
    rel = lambda i, me: (i ^ me[0], 0)
    whole = lambda i, me: (0, 0)
    q = pl.BlockSpec((BLOCK, wide), rel)
    k = pl.BlockSpec((tokens, HEAD), lambda i, me: (0, heads))
    v = pl.BlockSpec((tokens, HEAD), lambda i, me: (0, heads + 1))
    table = pl.BlockSpec((tokens, HEAD), whole)
    lse = pl.BlockSpec((heads, BLOCK), lambda i, me: (0, i))
    return q, k, v, table, lse, whole


def attend(me, qkv, cos, sin):
    tokens = qkv.shape[0]
    heads = qkv.shape[1] // HEAD - 2
    q, k, v, table, lse, _ = _attn_specs(tokens, heads)
    blocks = tokens // BLOCK
    return pl.pallas_call(
        functools.partial(_attn_fwd, heads=heads, blocks=blocks, scale=HEAD**-0.5),
        grid_spec=pltpu.PrefetchScalarGridSpec(
            num_scalar_prefetch=1, grid=(blocks,), in_specs=[q, k, v, table, table], out_specs=[q, lse],
            scratch_shapes=[pltpu.VMEM((tokens, HEAD), bf16), pltpu.VMEM((heads, BLOCK, HEAD), bf16), pltpu.VMEM((heads, BLOCK), f32),
                            pltpu.VMEM((heads, HEAD + 8, BLOCK), f32)],
        ),
        out_shape=[jax.ShapeDtypeStruct((tokens, heads * HEAD), bf16), jax.ShapeDtypeStruct((heads, tokens), f32)],
        compiler_params=pltpu.CompilerParams(dimension_semantics=("arbitrary",), vmem_limit_bytes=VMEM),
        cost_estimate=pl.CostEstimate(flops=2 * heads * tokens * tokens * HEAD * 4, transcendentals=heads * tokens * tokens, bytes_accessed=qkv.size * 4),
    )(me, qkv, qkv, qkv, cos, sin)


def attend_bwd(me, qkv, cos, sin, out, d_out, lse):
    tokens = qkv.shape[0]
    heads = qkv.shape[1] // HEAD - 2
    q, k, v, table, stats, whole = _attn_specs(tokens, heads)
    blocks = tokens // BLOCK
    return pl.pallas_call(
        functools.partial(_attn_bwd, heads=heads, blocks=blocks, scale=HEAD**-0.5),
        grid_spec=pltpu.PrefetchScalarGridSpec(
            num_scalar_prefetch=1, grid=(blocks,), in_specs=[q, k, v, table, table, q, q, stats], out_specs=pl.BlockSpec(qkv.shape, whole),
            scratch_shapes=[pltpu.VMEM((tokens, HEAD), bf16), pltpu.VMEM((heads, BLOCK, HEAD), bf16), pltpu.VMEM((heads, BLOCK), f32),
                            pltpu.VMEM((heads, HEAD, BLOCK), f32), pltpu.VMEM((tokens, HEAD), f32), pltpu.VMEM((tokens, HEAD), f32)],
        ),
        out_shape=jax.ShapeDtypeStruct(qkv.shape, bf16),
        compiler_params=pltpu.CompilerParams(dimension_semantics=("arbitrary",), vmem_limit_bytes=VMEM),
        cost_estimate=pl.CostEstimate(flops=2 * heads * tokens * tokens * HEAD * 6, transcendentals=heads * tokens * tokens, bytes_accessed=qkv.size * 8),
    )(me, qkv, qkv, qkv, cos, sin, out, d_out, lse)


FLIPS = {n: [(i, i ^ n) for i in range(4)] for n in (1, 2)}


def flip(t, axis, n):
    return lax.ppermute(t, axis, FLIPS[n])


def after(t, *others):
    return lax.optimization_barrier((t, *others))[0]


def gather(w):
    half = w.shape[0] // 2
    z, y = flip(w, "dp", 1), flip(w, "dp", 2)
    first = flip(z[:half], "dp", 2)
    second = flip(y[half:], "dp", 1)
    return w, z, y, first, second


def scatter(g, p):
    n = g.shape[0] // 4
    h = n // 2
    run = lambda j, at, size: lax.dynamic_slice_in_dim(g, (p ^ j) * n + at, size, axis=0)
    by_y = flip(run(3, 0, h), "dp", 2)
    by_z = flip(run(3, h, h), "dp", 1)
    got_z = flip(jnp.concatenate([add(run(1, 0, h), by_y), run(1, h, h)]), "dp", 1)
    got_y = flip(jnp.concatenate([run(2, 0, h), add(run(2, h, h), by_z)]), "dp", 2)
    return add(run(0, 0, n), got_z, got_y)


def add(*terms):
    return sum(t.astype(f32) for t in terms).astype(bf16)


def pair(own, mate, me):
    first = (jnp.arange(2) == me % 2)[:, None, None]
    return jnp.where(first, own[None], mate[None]).reshape(-1, own.shape[1])


def spread(t, me, *before):
    other = flip(t, "tp", 2)
    mate = flip(t, "tp", 1)
    near = pair(t, mate, me)

    def far(*others):
        got = after(other, *before)
        last = flip(got, "tp", 1)
        return pair(*after((got, last), *others), me)

    return near, far


def collect(near, far, me):
    n = near.shape[0] // 2
    of = lambda t, core: lax.dynamic_slice_in_dim(t, core * n, n, axis=0)
    core = me % 2
    to_x = add(of(far, core), flip(of(far, 1 - core), "tp", 1))
    got = flip(to_x, "tp", 2)
    return add(of(near, core), flip(of(near, 1 - core), "tp", 1), got)


def dot(a, b, ca=1, cb=0):
    return _dot(a, b, ca, cb)


def mm(a, b, ca=1, cb=0):
    return dot(a, b, ca, cb).astype(bf16)


def rms(h):
    wide = h.astype(f32)
    return lax.rsqrt(jnp.mean(wide**2, -1, keepdims=True) + 1e-6)


def rms_bwd(h, scale, d):
    wide, d = h.astype(f32), d.astype(f32)
    return scale * d - wide * (scale**3 * jnp.mean(d * wide, -1, keepdims=True))


def whole(runs, p):
    n = runs[0].shape[0]
    full = jnp.zeros((4 * n, runs[0].shape[1]), runs[0].dtype)
    for j, run in enumerate(runs[:3]):
        full = lax.dynamic_update_slice_in_dim(full, run, (p ^ j) * n, axis=0)
    for i, run in enumerate(runs[3:]):
        full = lax.dynamic_update_slice_in_dim(full, run, (p ^ 3) * n + i * (n // 2), axis=0)
    return full


def solution(mesh):
    def layer(x, dy, wq, wk, wv, wo, w_gate, w_up, w_down):
        x, dy = x[0], dy[0]
        p, me = lax.axis_index("dp"), lax.axis_index("tp")
        tokens = 4 * x.shape[0]
        half = HEAD // 2
        angle = jnp.arange(tokens, dtype=f32)[:, None] * THETA ** (-jnp.arange(half, dtype=f32) / half)
        cos, sin = jnp.cos(angle), jnp.sin(angle)
        cos, sin = jnp.concatenate([cos, cos], -1), jnp.concatenate([-sin, sin], -1)
        me1 = (me // 2 * 2).astype(jnp.int32).reshape(1)

        both = lambda s, t: jnp.concatenate([s, t])
        m = x.shape[0]

        w_qkv = jnp.concatenate([wq, wk, wv], axis=1)
        runs = gather(w_qkv)
        w_o = lax.all_gather(wo, "dp", axis=0, tiled=True)
        dy_all = lax.all_gather(after(dy, runs[1]), "tp", axis=0, tiled=True)
        w_qkv = whole(runs, p)
        gates = [w_gate, flip(w_gate, "dp", 1), flip(w_gate, "dp", 2)]
        ups = [w_up, flip(w_up, "dp", 1), flip(w_up, "dp", 2)]

        s1 = rms(x)
        a = (x.astype(f32) * s1).astype(bf16)
        a_near, a_far = spread(a, me, w_qkv, cos, sin)
        qkv_near = mm(a_near, w_qkv)
        a_far = a_far(qkv_near)
        qkv = both(qkv_near, mm(a_far, w_qkv))
        heads, lse = attend(me1, qkv, cos, sin)
        o_far = mm(heads[2 * m :], w_o)
        o_near = mm(after(heads, o_far)[: 2 * m], w_o)
        gates.append(flip(after(gates[1], o_near), "dp", 2))
        ups.append(flip(after(ups[2], o_near), "dp", 1))
        w_g, w_u = whole(gates, p), whole(ups, p)
        w_d = lax.all_gather(after(w_down, gates[3]), "dp", axis=0, tiled=True)
        h = x + collect(o_near, o_far, me)
        s2 = rms(h)
        b = (h.astype(f32) * s2).astype(bf16)
        chip = me // 2
        dy_near, dy_far = (lax.dynamic_slice_in_dim(dy_all, c * 2 * m, 2 * m, axis=0) for c in (chip, 1 - chip))
        b_near, b_far = spread(b, me, w_g, w_u, dy_near, dy_far)

        def first_dot(b):
            return dot(b, w_g)

        def up_and_hidden(b, gate):
            up = dot(b, w_u)
            return up, (jax.nn.silu(gate) * up).astype(bf16)

        def hidden_bwd(dy, gate, up):
            d_hid = mm(dy, w_d, 1, 1).astype(f32)
            sig = jax.nn.sigmoid(gate)
            silu = gate * sig
            return (d_hid * up * (sig + silu * (1 - sig))).astype(bf16), (d_hid * silu).astype(bf16)

        def db(dg, du):
            return (dot(dg, w_g, 1, 1) + dot(du, w_u, 1, 1)).astype(bf16)

        gate_near = first_dot(b_near)
        up_near, hid_near = up_and_hidden(after(b_near, gate_near), gate_near)
        b_far = b_far(hid_near)
        gate_far = first_dot(b_far)
        up_far, hid_far = up_and_hidden(after(b_far, gate_far), gate_far)
        dy_all = both(dy_near, dy_far)
        g_down = mm(both(hid_near, hid_far), dy_all, 0, 0)
        dg_far, du_far = hidden_bwd(after(dy_far, g_down), gate_far, up_far)
        db_far = db(dg_far, du_far)
        dg_near, du_near = hidden_bwd(after(dy_near, db_far), gate_near, up_near)
        b_all = both(b_near, b_far)
        g_gate = mm(b_all, both(dg_near, dg_far), 0, 0)
        db_near = db(*after((dg_near, du_near), g_gate))
        d_b = collect(db_near, db_far, me)
        d_h = dy + rms_bwd(h, s2, d_b).astype(bf16)
        dh_near, dh_far = spread(d_h, me)
        g_up = mm(b_all, after(both(du_near, du_far), d_h), 0, 0)
        do_near = mm(after(dh_near, g_up), w_o, 1, 1)
        dh_far = dh_far(do_near)
        do = both(do_near, mm(dh_far, w_o, 1, 1))
        d_qkv = attend_bwd(me1, qkv, cos, sin, heads, do, lse)
        da_far = mm(d_qkv[2 * m :], w_qkv, 1, 1)
        g_o = mm(after(heads, da_far), both(dh_near, dh_far), 0, 0)
        da_near = mm(after(d_qkv, g_o)[: 2 * m], w_qkv, 1, 1)
        g_qkv = mm(both(a_near, a_far), after(d_qkv, da_near), 0, 0)
        d_a = collect(da_near, da_far, me)
        d_x = d_h + rms_bwd(x, s1, d_a).astype(bf16)

        def total(g):
            return lax.psum_scatter(g, "dp", scatter_dimension=0, tiled=True)

        r_down, r_gate, r_up, r_o = (total(g) for g in (g_down, g_gate, g_up, g_o))
        r_qkv = scatter(g_qkv, p)
        cut = wq.shape[1]
        r_q, r_k, r_v = r_qkv[:, :cut], r_qkv[:, cut : cut + HEAD], r_qkv[:, cut + HEAD :]
        return d_x[None], r_q, r_k, r_v, r_o, r_gate, r_up, r_down

    states, by_columns, by_rows = P("dp", "tp", None), P("dp", "tp"), P(("tp", "dp"), None)
    weights = (by_columns, by_columns, by_columns, by_rows, by_columns, by_columns, by_rows)
    return jax.shard_map(layer, mesh=mesh, in_specs=(states, states, *weights), out_specs=(states, *weights), check_vma=False)
```

```python
import functools

import jax
import jax.numpy as jnp
from jax import lax
from jax.experimental import pallas as pl
from jax.experimental.pallas import tpu as pltpu
from jax.sharding import PartitionSpec as P


HEAD = 128
THETA = 10000
NEG = -1e30
HIDDEN = 2 * NEG
LOG2E = 1.4426950408889634
VMEM = 56 * 2**20
BLOCK = 512
f32, bf16 = jnp.float32, jnp.bfloat16


def _dot(a, b, ca, cb):
    return lax.dot_general(a, b, (((ca,), (cb,)), ((), ())), preferred_element_type=f32)


def _turn(t, cos, sin):
    return t * cos + pltpu.roll(t, HEAD // 2, 1) * sin


def _attn_fwd(me_ref, q_ref, k_ref, v_ref, cos_ref, sin_ref, o_ref, lse_ref, k_s, q_s, top_s, mix_s, *, heads, blocks, scale):
    me, iq = me_ref[0], pl.program_id(0)
    e = scale * LOG2E
    n = BLOCK

    @pl.when(iq == 0)
    def _():
        for j in range(blocks):
            rows = pl.ds(pl.multiple_of((j ^ me) * n, n), n)
            here = slice(j * n, (j + 1) * n)
            k_s[here, :] = _turn(k_ref[rows, :].astype(f32), cos_ref[here, :], sin_ref[here, :]).astype(bf16)

    mine = pl.ds(pl.multiple_of(iq * n, n), n)
    cos, sin = cos_ref[mine, :], sin_ref[mine, :]
    for h in range(heads):
        q_s[h] = _turn(q_ref[:, h * HEAD : (h + 1) * HEAD].astype(f32), cos, sin).astype(bf16)
    top_s[...] = jnp.full(top_s.shape, NEG, f32)
    mix_s[...] = jnp.zeros(mix_s.shape, f32)
    ones = jnp.ones((8, n), bf16)

    def block(j, masked):
        here = pl.ds(pl.multiple_of(j * n, n), n)
        rows = pl.ds(pl.multiple_of((j ^ me) * n, n), n)
        k = k_s[here, :]
        scores = [_dot(k, q_s[h], 1, 1) for h in range(heads)]
        if masked:
            ok = lax.broadcasted_iota(jnp.int32, (n, n), 1) >= lax.broadcasted_iota(jnp.int32, (n, n), 0)
        weights, keeps = [], []
        for h, s in enumerate(scores):
            if masked:
                s = jnp.where(ok, s, HIDDEN)
            old = top_s[h : h + 1, :]
            top = jnp.maximum(old, s.max(axis=0, keepdims=True))
            top_s[h : h + 1, :] = top
            weights.append(jnp.exp2((s - top) * e).astype(bf16))
            keeps.append(jnp.exp2((old - top) * e))
        values = jnp.concatenate([v_ref[rows, :].T, ones], axis=0)
        for h in range(heads):
            mix_s[h] = mix_s[h] * keeps[h] + _dot(values, weights[h], 1, 0)

    lax.fori_loop(0, iq, lambda j, _: block(j, False), None)
    block(iq, True)
    for h in range(heads):
        total = mix_s[h, HEAD : HEAD + 1, :]
        o_ref[:, h * HEAD : (h + 1) * HEAD] = (mix_s[h, :HEAD, :] * (1 / total)).T.astype(bf16)
        lse_ref[h : h + 1, :] = top_s[h : h + 1, :] * scale + jnp.log(total)


def _attn_bwd(me_ref, q_ref, k_ref, v_ref, cos_ref, sin_ref, o_ref, do_ref, lse_ref, d_ref, k_s, q_s, stat_s, dq_s, dk_s, dv_s, *, heads, blocks, scale):
    me, iq = me_ref[0], pl.program_id(0)
    e = scale * LOG2E
    n = BLOCK

    @pl.when(iq == 0)
    def _():
        for j in range(blocks):
            rows = pl.ds(pl.multiple_of((j ^ me) * n, n), n)
            here = slice(j * n, (j + 1) * n)
            k_s[here, :] = _turn(k_ref[rows, :].astype(f32), cos_ref[here, :], sin_ref[here, :]).astype(bf16)
        dk_s[...] = jnp.zeros_like(dk_s)
        dv_s[...] = jnp.zeros_like(dv_s)

    mine = pl.ds(pl.multiple_of(iq * n, n), n)
    cos, sin = cos_ref[mine, :], sin_ref[mine, :]
    for h in range(heads):
        cols = slice(h * HEAD, (h + 1) * HEAD)
        q_s[h] = _turn(q_ref[:, cols].astype(f32), cos, sin).astype(bf16)
        both = (do_ref[:, cols].astype(f32) * o_ref[:, cols].astype(f32)).T
        stat_s[h : h + 1, :] = both.sum(axis=0, keepdims=True)
    dq_s[...] = jnp.zeros_like(dq_s)

    def block(j, masked):
        here = pl.ds(pl.multiple_of(j * n, n), n)
        rows = pl.ds(pl.multiple_of((j ^ me) * n, n), n)
        k, v = k_s[here, :], v_ref[rows, :]
        dos = [do_ref[:, h * HEAD : (h + 1) * HEAD] for h in range(heads)]
        scores = [_dot(k, q_s[h], 1, 1) for h in range(heads)]
        dps = [_dot(v, dos[h], 1, 1) for h in range(heads)]
        kt = k.T
        if masked:
            ok = lax.broadcasted_iota(jnp.int32, (n, n), 1) >= lax.broadcasted_iota(jnp.int32, (n, n), 0)
        for h in range(heads):
            p = jnp.exp2(scores[h] * e - lse_ref[h : h + 1, :] * LOG2E)
            if masked:
                p = jnp.where(ok, p, 0.0)
            ds = (p * (dps[h] - stat_s[h : h + 1, :])).astype(bf16)
            dv_s[here, :] += _dot(p.astype(bf16), dos[h], 1, 0)
            dk_s[here, :] += _dot(ds, q_s[h], 1, 0)
            dq_s[h] += _dot(kt, ds, 1, 0)

    lax.fori_loop(0, iq, lambda j, _: block(j, False), None)
    block(iq, True)
    place = pl.ds(pl.multiple_of((iq ^ me) * n, n), n)
    for h in range(heads):
        d_ref[place, h * HEAD : (h + 1) * HEAD] = _turn((dq_s[h] * scale).T, cos, -sin).astype(bf16)

    @pl.when(iq == blocks - 1)
    def _():
        at = heads * HEAD
        for j in range(blocks):
            rows = pl.ds(pl.multiple_of((j ^ me) * n, n), n)
            here = slice(j * n, (j + 1) * n)
            d_ref[rows, at : at + HEAD] = _turn(dk_s[here, :] * scale, cos_ref[here, :], -sin_ref[here, :]).astype(bf16)
            d_ref[rows, at + HEAD : at + 2 * HEAD] = dv_s[here, :].astype(bf16)


def _attn_specs(tokens, heads):
    wide = heads * HEAD
    rel = lambda i, me: (i ^ me[0], 0)
    whole = lambda i, me: (0, 0)
    q = pl.BlockSpec((BLOCK, wide), rel)
    k = pl.BlockSpec((tokens, HEAD), lambda i, me: (0, heads))
    v = pl.BlockSpec((tokens, HEAD), lambda i, me: (0, heads + 1))
    table = pl.BlockSpec((tokens, HEAD), whole)
    lse = pl.BlockSpec((heads, BLOCK), lambda i, me: (0, i))
    return q, k, v, table, lse, whole


def attend(me, qkv, cos, sin):
    tokens = qkv.shape[0]
    heads = qkv.shape[1] // HEAD - 2
    q, k, v, table, lse, _ = _attn_specs(tokens, heads)
    blocks = tokens // BLOCK
    return pl.pallas_call(
        functools.partial(_attn_fwd, heads=heads, blocks=blocks, scale=HEAD**-0.5),
        grid_spec=pltpu.PrefetchScalarGridSpec(
            num_scalar_prefetch=1, grid=(blocks,), in_specs=[q, k, v, table, table], out_specs=[q, lse],
            scratch_shapes=[pltpu.VMEM((tokens, HEAD), bf16), pltpu.VMEM((heads, BLOCK, HEAD), bf16), pltpu.VMEM((heads, BLOCK), f32),
                            pltpu.VMEM((heads, HEAD + 8, BLOCK), f32)],
        ),
        out_shape=[jax.ShapeDtypeStruct((tokens, heads * HEAD), bf16), jax.ShapeDtypeStruct((heads, tokens), f32)],
        compiler_params=pltpu.CompilerParams(dimension_semantics=("arbitrary",), vmem_limit_bytes=VMEM),
        cost_estimate=pl.CostEstimate(flops=2 * heads * tokens * tokens * HEAD * 4, transcendentals=heads * tokens * tokens, bytes_accessed=qkv.size * 4),
    )(me, qkv, qkv, qkv, cos, sin)


def attend_bwd(me, qkv, cos, sin, out, d_out, lse):
    tokens = qkv.shape[0]
    heads = qkv.shape[1] // HEAD - 2
    q, k, v, table, stats, whole = _attn_specs(tokens, heads)
    blocks = tokens // BLOCK
    return pl.pallas_call(
        functools.partial(_attn_bwd, heads=heads, blocks=blocks, scale=HEAD**-0.5),
        grid_spec=pltpu.PrefetchScalarGridSpec(
            num_scalar_prefetch=1, grid=(blocks,), in_specs=[q, k, v, table, table, q, q, stats], out_specs=pl.BlockSpec(qkv.shape, whole),
            scratch_shapes=[pltpu.VMEM((tokens, HEAD), bf16), pltpu.VMEM((heads, BLOCK, HEAD), bf16), pltpu.VMEM((heads, BLOCK), f32),
                            pltpu.VMEM((heads, HEAD, BLOCK), f32), pltpu.VMEM((tokens, HEAD), f32), pltpu.VMEM((tokens, HEAD), f32)],
        ),
        out_shape=jax.ShapeDtypeStruct(qkv.shape, bf16),
        compiler_params=pltpu.CompilerParams(dimension_semantics=("arbitrary",), vmem_limit_bytes=VMEM),
        cost_estimate=pl.CostEstimate(flops=2 * heads * tokens * tokens * HEAD * 6, transcendentals=heads * tokens * tokens, bytes_accessed=qkv.size * 8),
    )(me, qkv, qkv, qkv, cos, sin, out, d_out, lse)


TILE = 256
RUNS = 4


def _call(body, p, grid, args, specs, outs, out_specs, flops):
    return pl.pallas_call(
        body,
        grid_spec=pltpu.PrefetchScalarGridSpec(num_scalar_prefetch=1, grid=(grid,), in_specs=specs, out_specs=out_specs),
        out_shape=outs,
        compiler_params=pltpu.CompilerParams(dimension_semantics=("arbitrary",), vmem_limit_bytes=VMEM),
        cost_estimate=pl.CostEstimate(flops=flops, transcendentals=0, bytes_accessed=sum(a.size * a.dtype.itemsize for a in args)),
    )(p, *args)


def _by_runs(p_ref, b_ref, runs):
    total, n = None, runs[0].shape[0]
    for i, run in enumerate(runs):
        j, at = (i, 0) if i < RUNS else (RUNS - 1, n // 2)
        size = run.shape[0]
        part = _dot(b_ref[:, pl.ds(pl.multiple_of((p_ref[0] ^ j) * n + at, size), size)], run[...], 1, 0)
        total = part if total is None else total + part
    return total


def _gate(p_ref, b_ref, *refs):
    refs[-1][...] = _by_runs(p_ref, b_ref, refs[:-1])


def _up(p_ref, b_ref, gate_ref, *refs):
    *ups, up_ref, hid_ref = refs
    gate = gate_ref[...]
    up = _by_runs(p_ref, b_ref, ups)
    up_ref[...] = up
    hid_ref[...] = (gate * jax.nn.sigmoid(gate) * up).astype(bf16)


def _gate_up(p_ref, b_ref, *refs):
    gates, ups, (gate_ref, up_ref, hid_ref) = refs[: RUNS + 1], refs[RUNS + 1 : -3], refs[-3:]
    gate = _by_runs(p_ref, b_ref, gates)
    up = _by_runs(p_ref, b_ref, ups)
    gate_ref[...] = gate
    up_ref[...] = up
    hid_ref[...] = (gate * jax.nn.sigmoid(gate) * up).astype(bf16)


def gate_up(p, b, gates=(), ups=(), gate=None):
    tokens, d = b.shape
    runs = (*gates, *ups)
    ff = runs[0].shape[1]
    tile = pl.BlockSpec((tokens, TILE), lambda i, p: (0, i))
    wide, narrow = (jax.ShapeDtypeStruct((tokens, ff), t) for t in (f32, bf16))
    whole = pl.BlockSpec((tokens, d), lambda i, p: (0, 0))
    specs = [pl.BlockSpec((run.shape[0], TILE), lambda i, p: (0, i)) for run in runs]
    flops = 2 * tokens * d * ff
    if not ups:
        return _call(_gate, p, ff // TILE, (b, *runs), [whole, *specs], wide, tile, flops)
    if not gates:
        return _call(_up, p, ff // TILE, (b, gate, *runs), [whole, tile, *specs], [wide, narrow], [tile] * 2, flops)
    return _call(_gate_up, p, ff // TILE, (b, *runs), [whole, *specs], [wide, wide, narrow], [tile] * 3, 2 * flops)


def _hidden_bwd(p_ref, dy_ref, w_ref, gate_ref, up_ref, dg_ref, du_ref):
    for at in range(0, gate_ref.shape[0], 256):
        rows = slice(at, at + 256)
        d_hid = _dot(dy_ref[rows, :], w_ref[...], 1, 1).astype(bf16).astype(f32)
        gate = gate_ref[rows, :]
        sig = jax.nn.sigmoid(gate)
        silu = gate * sig
        dg_ref[rows, :] = (d_hid * up_ref[rows, :] * (sig + silu * (1 - sig))).astype(bf16)
        du_ref[rows, :] = (d_hid * silu).astype(bf16)


def hidden_bwd(p, dy, w_d, gate, up):
    tokens, ff = gate.shape
    d = dy.shape[1]
    wide = 2 * TILE
    tile = pl.BlockSpec((tokens, wide), lambda i, p: (0, i))
    shape = jax.ShapeDtypeStruct((tokens, ff), bf16)
    return _call(_hidden_bwd, p, ff // wide, (dy, w_d, gate, up),
                 [pl.BlockSpec((tokens, d), lambda i, p: (0, 0)), pl.BlockSpec((wide, d), lambda i, p: (i, 0)), tile, tile],
                 [shape, shape], [tile, tile], 2 * tokens * d * ff)


def _norm_bwd(starts, p_ref, dg_ref, du_ref, *refs):
    *runs, o_ref = refs
    gates, ups = runs[: RUNS + 1], runs[RUNS + 1 :]
    i = pl.program_id(0)
    for k in range(RUNS + 1):

        @pl.when((i >= starts[k]) & (i < starts[k + 1]))
        def _():
            o_ref[...] = (_dot(dg_ref[...], gates[k][...], 1, 1) + _dot(du_ref[...], ups[k][...], 1, 1)).astype(bf16)


def norm_bwd(p, dg, du, gates, ups):
    tokens, ff = dg.shape
    n = gates[0].shape[0]
    d = RUNS * n
    per = n // TILE
    starts = [0]
    for run in gates:
        starts.append(starts[-1] + run.shape[0] // TILE)
    whole = pl.BlockSpec((tokens, ff), lambda i, p: (0, 0))
    runs = [pl.BlockSpec((TILE, ff), lambda i, p, s=s, e=e: (jnp.clip(i - s, 0, e - s - 1), 0)) for s, e in zip(starts, starts[1:])]
    return _call(functools.partial(_norm_bwd, starts), p, RUNS * per, (dg, du, *gates, *ups), [whole, whole, *runs, *runs],
                 jax.ShapeDtypeStruct((tokens, d), bf16), pl.BlockSpec((tokens, TILE), lambda i, p: (0, (i // per ^ p[0]) * per + i % per)),
                 4 * tokens * d * ff)


def _by_weight(p_ref, a_near, a_far, b_near, b_far, o_ref):
    for at in range(0, o_ref.shape[1], 512):
        cols = slice(at, at + 512)
        o_ref[:, cols] = (_dot(a_near[...], b_near[:, cols], 0, 0) + _dot(a_far[...], b_far[:, cols], 0, 0)).astype(bf16)


def by_weight(p, a_near, a_far, b_near, b_far, part=None):
    tokens, rows = a_near.shape
    cols, at = (b_near.shape[1], 0) if part is None else (b_near.shape[1] // 2, part)
    tile = pl.BlockSpec((tokens, TILE), lambda i, p: (0, i))
    columns = pl.BlockSpec((tokens, cols), lambda i, p: (0, at))
    return _call(_by_weight, p, rows // TILE, (a_near, a_far, b_near, b_far),
                 [tile, tile, columns, columns], jax.ShapeDtypeStruct((rows, cols), bf16),
                 pl.BlockSpec((TILE, cols), lambda i, p: (i, 0)), 4 * tokens * rows * cols)


FLIPS = {n: [(i, i ^ n) for i in range(4)] for n in (1, 2)}


def flip(t, axis, n):
    return lax.ppermute(t, axis, FLIPS[n])


def after(t, *others):
    return lax.optimization_barrier((t, *others))[0]


def gather(w):
    half = w.shape[0] // 2
    z, y = flip(w, "dp", 1), flip(w, "dp", 2)

    def far(*before):
        first = flip(after(z, *before)[:half], "dp", 2)
        second = flip(after(y, *before)[half:], "dp", 1)
        return w, z, y, first, second

    return far


def scatter(g, p):
    n = g.shape[0] // 4
    h = n // 2
    run = lambda j, at, size: lax.dynamic_slice_in_dim(g, (p ^ j) * n + at, size, axis=0)
    by_y = flip(run(3, 0, h), "dp", 2)
    by_z = flip(run(3, h, h), "dp", 1)
    got_z = flip(jnp.concatenate([add(run(1, 0, h), by_y), run(1, h, h)]), "dp", 1)
    got_y = flip(jnp.concatenate([run(2, 0, h), add(run(2, h, h), by_z)]), "dp", 2)
    return add(run(0, 0, n), got_z, got_y)


def add(*terms):
    return sum(t.astype(f32) for t in terms).astype(bf16)


def pair(own, mate, me):
    first = (jnp.arange(2) == me % 2)[:, None, None]
    return jnp.where(first, own[None], mate[None]).reshape(-1, own.shape[1])


def spread(t, me, *before):
    other = flip(t, "tp", 2)
    mate = flip(t, "tp", 1)
    near = pair(t, mate, me)

    def far(*others):
        got = after(other, *before)
        last = flip(got, "tp", 1)
        return pair(*after((got, last), *others), me)

    return near, far


def collect(near, far, me):
    n = near.shape[0] // 2
    of = lambda t, core: lax.dynamic_slice_in_dim(t, core * n, n, axis=0)
    core = me % 2
    to_x = add(of(far, core), flip(of(far, 1 - core), "tp", 1))
    got = flip(to_x, "tp", 2)
    return add(of(near, core), flip(of(near, 1 - core), "tp", 1), got)


def dot(a, b, ca=1, cb=0):
    return _dot(a, b, ca, cb)


def mm(a, b, ca=1, cb=0):
    return dot(a, b, ca, cb).astype(bf16)


def rms(h):
    wide = h.astype(f32)
    return lax.rsqrt(jnp.mean(wide**2, -1, keepdims=True) + 1e-6)


def rms_bwd(h, scale, d):
    wide, d = h.astype(f32), d.astype(f32)
    return scale * d - wide * (scale**3 * jnp.mean(d * wide, -1, keepdims=True))


def whole(runs, p):
    n = runs[0].shape[0]
    full = jnp.zeros((4 * n, runs[0].shape[1]), runs[0].dtype)
    for j, run in enumerate(runs[:3]):
        full = lax.dynamic_update_slice_in_dim(full, run, (p ^ j) * n, axis=0)
    for i, run in enumerate(runs[3:]):
        full = lax.dynamic_update_slice_in_dim(full, run, (p ^ 3) * n + i * (n // 2), axis=0)
    return full


def solution(mesh):
    def layer(x, dy, wq, wk, wv, wo, w_gate, w_up, w_down):
        x, dy = x[0], dy[0]
        p, me = lax.axis_index("dp"), lax.axis_index("tp")
        tokens = 4 * x.shape[0]
        half = HEAD // 2
        angle = jnp.arange(tokens, dtype=f32)[:, None] * THETA ** (-jnp.arange(half, dtype=f32) / half)
        cos, sin = jnp.cos(angle), jnp.sin(angle)
        cos, sin = jnp.concatenate([cos, cos], -1), jnp.concatenate([-sin, sin], -1)
        me1 = (me // 2 * 2).astype(jnp.int32).reshape(1)

        both = lambda s, t: jnp.concatenate([s, t])
        m = x.shape[0]

        w_qkv = jnp.concatenate([wq, wk, wv], axis=1)
        w_o = whole(gather(wo)(), p)
        runs = gather(w_qkv)()
        dy_other = flip(dy, "tp", 2)
        w_qkv = whole(runs, p)
        gates, ups = gather(w_gate), gather(w_up)

        s1 = rms(x)
        a = (x.astype(f32) * s1).astype(bf16)
        a_near, a_far = spread(a, me, w_qkv, cos, sin)
        qkv_near = mm(a_near, w_qkv)
        a_far = a_far(qkv_near)
        qkv = both(qkv_near, mm(a_far, w_qkv))
        heads, lse = attend(me1, qkv, cos, sin)
        o_far = mm(heads[2 * m :], w_o)
        o_near = mm(after(heads, o_far)[: 2 * m], w_o)
        gates, ups = gates(o_near), ups(o_near)
        h = x + collect(o_near, o_far, me)
        s2 = rms(h)
        b = (h.astype(f32) * s2).astype(bf16)
        dy_near = pair(dy, flip(after(dy, o_near), "tp", 1), me)
        dy_far = pair(dy_other, flip(after(dy_other, o_near), "tp", 1), me)
        place = p.astype(jnp.int32).reshape(1)
        b_near, b_far = spread(b, me)
        w_d = lax.all_gather(after(w_down, b_near), "dp", axis=0, tiled=True)
        gate_near = gate_up(place, b_near, gates=gates)
        up_near, hid_near = gate_up(place, b_near, ups=ups, gate=gate_near)
        b_far = b_far(hid_near)
        gate_far, up_far, hid_far = gate_up(place, b_far, gates, ups)
        g_down = by_weight(place, hid_near, hid_far, dy_near, dy_far)
        dg_far, du_far = hidden_bwd(place, after(dy_far, g_down), w_d, gate_far, up_far)
        db_far = norm_bwd(place, dg_far, du_far, gates, ups)
        dg_near, du_near = hidden_bwd(place, after(dy_near, db_far), w_d, gate_near, up_near)
        g_gate_1 = by_weight(place, b_near, b_far, dg_near, dg_far, part=0)
        db_near = norm_bwd(place, *after((dg_near, du_near), g_gate_1), gates, ups)
        d_b = collect(db_near, db_far, me)
        d_h = dy + rms_bwd(h, s2, d_b).astype(bf16)
        dh_near, dh_far = spread(d_h, me)
        g_gate_2 = by_weight(place, b_near, b_far, after(dg_near, d_h), dg_far, part=1)
        g_up = by_weight(place, b_near, b_far, after(du_near, g_gate_2), du_far)
        do_near = mm(after(dh_near, g_up), w_o, 1, 1)
        dh_far = dh_far(do_near)
        do = both(do_near, mm(dh_far, w_o, 1, 1))
        d_qkv = attend_bwd(me1, qkv, cos, sin, heads, do, lse)
        da_far = mm(d_qkv[2 * m :], w_qkv, 1, 1)
        g_o = mm(heads, both(dh_near, dh_far), 0, 0)
        g_qkv = mm(both(a_near, a_far), after(d_qkv, da_far), 0, 0)
        da_near = mm(after(d_qkv, g_qkv)[: 2 * m], w_qkv, 1, 1)
        d_a = collect(da_near, da_far, me)
        d_x = (d_h + rms_bwd(x, s1, d_a).astype(bf16))[None]

        def total(g):
            return lax.psum_scatter(g, "dp", scatter_dimension=0, tiled=True)

        r_down, r_up, r_o = total(g_down), total(g_up), scatter(g_o, p)
        r_gate = jnp.concatenate([total(g_gate_1), total(g_gate_2)], axis=1)
        r_qkv = scatter(g_qkv, p)
        cut = wq.shape[1]
        r_q, r_k, r_v = r_qkv[:, :cut], r_qkv[:, cut : cut + HEAD], r_qkv[:, cut + HEAD :]
        return d_x, r_q, r_k, r_v, r_o, r_gate, r_up, r_down

    states, by_columns, by_rows = P("dp", "tp", None), P("dp", "tp"), P(("tp", "dp"), None)
    weights = (by_columns, by_columns, by_columns, by_rows, by_columns, by_columns, by_rows)
    return jax.shard_map(layer, mesh=mesh, in_specs=(states, states, *weights), out_specs=(states, *weights), check_vma=False)
```

```python
import functools

import jax
import jax.numpy as jnp
from jax import lax
from jax.experimental import pallas as pl
from jax.experimental.pallas import tpu as pltpu
from jax.sharding import PartitionSpec as P


HEAD = 128
THETA = 10000
NEG = -1e30
HIDDEN = 2 * NEG
LOG2E = 1.4426950408889634
VMEM = 56 * 2**20
BLOCK = 512
f32, bf16 = jnp.float32, jnp.bfloat16


def _dot(a, b, ca, cb):
    return lax.dot_general(a, b, (((ca,), (cb,)), ((), ())), preferred_element_type=f32)


def _turn(t, cos, sin):
    return t * cos + pltpu.roll(t, HEAD // 2, 1) * sin


def _attn_fwd(me_ref, q_ref, k_ref, v_ref, cos_ref, sin_ref, o_ref, lse_ref, k_s, q_s, top_s, mix_s, *, heads, blocks, scale):
    me, iq = me_ref[0], pl.program_id(0)
    e = scale * LOG2E
    n = BLOCK

    @pl.when(iq == 0)
    def _():
        for j in range(blocks):
            rows = pl.ds(pl.multiple_of((j ^ me) * n, n), n)
            here = slice(j * n, (j + 1) * n)
            k_s[here, :] = _turn(k_ref[rows, :].astype(f32), cos_ref[here, :], sin_ref[here, :]).astype(bf16)

    mine = pl.ds(pl.multiple_of(iq * n, n), n)
    cos, sin = cos_ref[mine, :], sin_ref[mine, :]
    for h in range(heads):
        q_s[h] = _turn(q_ref[:, h * HEAD : (h + 1) * HEAD].astype(f32), cos, sin).astype(bf16)
    top_s[...] = jnp.full(top_s.shape, NEG, f32)
    mix_s[...] = jnp.zeros(mix_s.shape, f32)
    ones = jnp.ones((8, n), bf16)

    def block(j, masked):
        here = pl.ds(pl.multiple_of(j * n, n), n)
        rows = pl.ds(pl.multiple_of((j ^ me) * n, n), n)
        k = k_s[here, :]
        scores = [_dot(k, q_s[h], 1, 1) for h in range(heads)]
        if masked:
            ok = lax.broadcasted_iota(jnp.int32, (n, n), 1) >= lax.broadcasted_iota(jnp.int32, (n, n), 0)
        weights, keeps = [], []
        for h, s in enumerate(scores):
            if masked:
                s = jnp.where(ok, s, HIDDEN)
            old = top_s[h : h + 1, :]
            top = jnp.maximum(old, s.max(axis=0, keepdims=True))
            top_s[h : h + 1, :] = top
            weights.append(jnp.exp2((s - top) * e).astype(bf16))
            keeps.append(jnp.exp2((old - top) * e))
        values = jnp.concatenate([v_ref[rows, :].T, ones], axis=0)
        for h in range(heads):
            mix_s[h] = mix_s[h] * keeps[h] + _dot(values, weights[h], 1, 0)

    lax.fori_loop(0, iq, lambda j, _: block(j, False), None)
    block(iq, True)
    for h in range(heads):
        total = mix_s[h, HEAD : HEAD + 1, :]
        o_ref[:, h * HEAD : (h + 1) * HEAD] = (mix_s[h, :HEAD, :] * (1 / total)).T.astype(bf16)
        lse_ref[h : h + 1, :] = top_s[h : h + 1, :] * scale + jnp.log(total)


def _attn_bwd(me_ref, q_ref, k_ref, v_ref, cos_ref, sin_ref, o_ref, do_ref, lse_ref, d_ref, k_s, q_s, stat_s, dq_s, dk_s, dv_s, *, heads, blocks, scale):
    me, iq = me_ref[0], pl.program_id(0)
    e = scale * LOG2E
    n = BLOCK

    @pl.when(iq == 0)
    def _():
        for j in range(blocks):
            rows = pl.ds(pl.multiple_of((j ^ me) * n, n), n)
            here = slice(j * n, (j + 1) * n)
            k_s[here, :] = _turn(k_ref[rows, :].astype(f32), cos_ref[here, :], sin_ref[here, :]).astype(bf16)
        dk_s[...] = jnp.zeros_like(dk_s)
        dv_s[...] = jnp.zeros_like(dv_s)

    mine = pl.ds(pl.multiple_of(iq * n, n), n)
    cos, sin = cos_ref[mine, :], sin_ref[mine, :]
    for h in range(heads):
        cols = slice(h * HEAD, (h + 1) * HEAD)
        q_s[h] = _turn(q_ref[:, cols].astype(f32), cos, sin).astype(bf16)
        both = (do_ref[:, cols].astype(f32) * o_ref[:, cols].astype(f32)).T
        stat_s[h : h + 1, :] = both.sum(axis=0, keepdims=True)
    dq_s[...] = jnp.zeros_like(dq_s)

    def block(j, masked):
        here = pl.ds(pl.multiple_of(j * n, n), n)
        rows = pl.ds(pl.multiple_of((j ^ me) * n, n), n)
        k, v = k_s[here, :], v_ref[rows, :]
        dos = [do_ref[:, h * HEAD : (h + 1) * HEAD] for h in range(heads)]
        scores = [_dot(k, q_s[h], 1, 1) for h in range(heads)]
        dps = [_dot(v, dos[h], 1, 1) for h in range(heads)]
        kt = k.T
        if masked:
            ok = lax.broadcasted_iota(jnp.int32, (n, n), 1) >= lax.broadcasted_iota(jnp.int32, (n, n), 0)
        for h in range(heads):
            p = jnp.exp2(scores[h] * e - lse_ref[h : h + 1, :] * LOG2E)
            if masked:
                p = jnp.where(ok, p, 0.0)
            ds = (p * (dps[h] - stat_s[h : h + 1, :])).astype(bf16)
            dv_s[here, :] += _dot(p.astype(bf16), dos[h], 1, 0)
            dk_s[here, :] += _dot(ds, q_s[h], 1, 0)
            dq_s[h] += _dot(kt, ds, 1, 0)

    lax.fori_loop(0, iq, lambda j, _: block(j, False), None)
    block(iq, True)
    place = pl.ds(pl.multiple_of((iq ^ me) * n, n), n)
    for h in range(heads):
        d_ref[place, h * HEAD : (h + 1) * HEAD] = _turn((dq_s[h] * scale).T, cos, -sin).astype(bf16)

    @pl.when(iq == blocks - 1)
    def _():
        at = heads * HEAD
        for j in range(blocks):
            rows = pl.ds(pl.multiple_of((j ^ me) * n, n), n)
            here = slice(j * n, (j + 1) * n)
            d_ref[rows, at : at + HEAD] = _turn(dk_s[here, :] * scale, cos_ref[here, :], -sin_ref[here, :]).astype(bf16)
            d_ref[rows, at + HEAD : at + 2 * HEAD] = dv_s[here, :].astype(bf16)


def _attn_specs(tokens, heads):
    wide = heads * HEAD
    rel = lambda i, me: (i ^ me[0], 0)
    whole = lambda i, me: (0, 0)
    q = pl.BlockSpec((BLOCK, wide), rel)
    k = pl.BlockSpec((tokens, HEAD), lambda i, me: (0, heads))
    v = pl.BlockSpec((tokens, HEAD), lambda i, me: (0, heads + 1))
    table = pl.BlockSpec((tokens, HEAD), whole)
    lse = pl.BlockSpec((heads, BLOCK), lambda i, me: (0, i))
    return q, k, v, table, lse, whole


def attend(me, qkv, cos, sin):
    tokens = qkv.shape[0]
    heads = qkv.shape[1] // HEAD - 2
    q, k, v, table, lse, _ = _attn_specs(tokens, heads)
    blocks = tokens // BLOCK
    return pl.pallas_call(
        functools.partial(_attn_fwd, heads=heads, blocks=blocks, scale=HEAD**-0.5),
        grid_spec=pltpu.PrefetchScalarGridSpec(
            num_scalar_prefetch=1, grid=(blocks,), in_specs=[q, k, v, table, table], out_specs=[q, lse],
            scratch_shapes=[pltpu.VMEM((tokens, HEAD), bf16), pltpu.VMEM((heads, BLOCK, HEAD), bf16), pltpu.VMEM((heads, BLOCK), f32),
                            pltpu.VMEM((heads, HEAD + 8, BLOCK), f32)],
        ),
        out_shape=[jax.ShapeDtypeStruct((tokens, heads * HEAD), bf16), jax.ShapeDtypeStruct((heads, tokens), f32)],
        compiler_params=pltpu.CompilerParams(dimension_semantics=("arbitrary",), vmem_limit_bytes=VMEM),
        cost_estimate=pl.CostEstimate(flops=2 * heads * tokens * tokens * HEAD * 4, transcendentals=heads * tokens * tokens, bytes_accessed=qkv.size * 4),
    )(me, qkv, qkv, qkv, cos, sin)


def attend_bwd(me, qkv, cos, sin, out, d_out, lse):
    tokens = qkv.shape[0]
    heads = qkv.shape[1] // HEAD - 2
    q, k, v, table, stats, whole = _attn_specs(tokens, heads)
    blocks = tokens // BLOCK
    return pl.pallas_call(
        functools.partial(_attn_bwd, heads=heads, blocks=blocks, scale=HEAD**-0.5),
        grid_spec=pltpu.PrefetchScalarGridSpec(
            num_scalar_prefetch=1, grid=(blocks,), in_specs=[q, k, v, table, table, q, q, stats], out_specs=pl.BlockSpec(qkv.shape, whole),
            scratch_shapes=[pltpu.VMEM((tokens, HEAD), bf16), pltpu.VMEM((heads, BLOCK, HEAD), bf16), pltpu.VMEM((heads, BLOCK), f32),
                            pltpu.VMEM((heads, HEAD, BLOCK), f32), pltpu.VMEM((tokens, HEAD), f32), pltpu.VMEM((tokens, HEAD), f32)],
        ),
        out_shape=jax.ShapeDtypeStruct(qkv.shape, bf16),
        compiler_params=pltpu.CompilerParams(dimension_semantics=("arbitrary",), vmem_limit_bytes=VMEM),
        cost_estimate=pl.CostEstimate(flops=2 * heads * tokens * tokens * HEAD * 6, transcendentals=heads * tokens * tokens, bytes_accessed=qkv.size * 8),
    )(me, qkv, qkv, qkv, cos, sin, out, d_out, lse)


TILE = 256
RUNS = 4


def _call(body, p, grid, args, specs, outs, out_specs, flops):
    return pl.pallas_call(
        body,
        grid_spec=pltpu.PrefetchScalarGridSpec(num_scalar_prefetch=1, grid=(grid,), in_specs=specs, out_specs=out_specs),
        out_shape=outs,
        compiler_params=pltpu.CompilerParams(dimension_semantics=("arbitrary",), vmem_limit_bytes=VMEM),
        cost_estimate=pl.CostEstimate(flops=flops, transcendentals=0, bytes_accessed=sum(a.size * a.dtype.itemsize for a in args)),
    )(p, *args)


def _by_runs(p_ref, b_ref, runs):
    total, n = None, runs[0].shape[0]
    for i, run in enumerate(runs):
        j, at = (i, 0) if i < RUNS else (RUNS - 1, n // 2)
        size = run.shape[0]
        part = _dot(b_ref[:, pl.ds(pl.multiple_of((p_ref[0] ^ j) * n + at, size), size)], run[...], 1, 0)
        total = part if total is None else total + part
    return total


def _gate(p_ref, b_ref, *refs):
    refs[-1][...] = _by_runs(p_ref, b_ref, refs[:-1])


def _up(p_ref, b_ref, gate_ref, *refs):
    *ups, up_ref, hid_ref = refs
    gate = gate_ref[...]
    up = _by_runs(p_ref, b_ref, ups)
    up_ref[...] = up
    hid_ref[...] = (gate * jax.nn.sigmoid(gate) * up).astype(bf16)


def _gate_up(p_ref, b_ref, *refs):
    gates, ups, (gate_ref, up_ref, hid_ref) = refs[: RUNS + 1], refs[RUNS + 1 : -3], refs[-3:]
    gate = _by_runs(p_ref, b_ref, gates)
    up = _by_runs(p_ref, b_ref, ups)
    gate_ref[...] = gate
    up_ref[...] = up
    hid_ref[...] = (gate * jax.nn.sigmoid(gate) * up).astype(bf16)


def gate_up(p, b, gates=(), ups=(), gate=None):
    tokens, d = b.shape
    runs = (*gates, *ups)
    ff = runs[0].shape[1]
    tile = pl.BlockSpec((tokens, TILE), lambda i, p: (0, i))
    wide, narrow = (jax.ShapeDtypeStruct((tokens, ff), t) for t in (f32, bf16))
    whole = pl.BlockSpec((tokens, d), lambda i, p: (0, 0))
    specs = [pl.BlockSpec((run.shape[0], TILE), lambda i, p: (0, i)) for run in runs]
    flops = 2 * tokens * d * ff
    if not ups:
        return _call(_gate, p, ff // TILE, (b, *runs), [whole, *specs], wide, tile, flops)
    if not gates:
        return _call(_up, p, ff // TILE, (b, gate, *runs), [whole, tile, *specs], [wide, narrow], [tile] * 2, flops)
    return _call(_gate_up, p, ff // TILE, (b, *runs), [whole, *specs], [wide, wide, narrow], [tile] * 3, 2 * flops)


def _hidden_bwd(p_ref, dy_ref, w_ref, gate_ref, up_ref, dg_ref, du_ref):
    for at in range(0, gate_ref.shape[0], 256):
        rows = slice(at, at + 256)
        d_hid = _dot(dy_ref[rows, :], w_ref[...], 1, 1).astype(bf16).astype(f32)
        gate = gate_ref[rows, :]
        sig = jax.nn.sigmoid(gate)
        silu = gate * sig
        dg_ref[rows, :] = (d_hid * up_ref[rows, :] * (sig + silu * (1 - sig))).astype(bf16)
        du_ref[rows, :] = (d_hid * silu).astype(bf16)


def hidden_bwd(p, dy, w_d, gate, up):
    tokens, ff = gate.shape
    d = dy.shape[1]
    wide = 2 * TILE
    tile = pl.BlockSpec((tokens, wide), lambda i, p: (0, i))
    shape = jax.ShapeDtypeStruct((tokens, ff), bf16)
    return _call(_hidden_bwd, p, ff // wide, (dy, w_d, gate, up),
                 [pl.BlockSpec((tokens, d), lambda i, p: (0, 0)), pl.BlockSpec((wide, d), lambda i, p: (i, 0)), tile, tile],
                 [shape, shape], [tile, tile], 2 * tokens * d * ff)


def _norm_bwd(starts, p_ref, dg_ref, du_ref, *refs):
    *runs, o_ref = refs
    gates, ups = runs[: RUNS + 1], runs[RUNS + 1 :]
    i = pl.program_id(0)
    for k in range(RUNS + 1):

        @pl.when((i >= starts[k]) & (i < starts[k + 1]))
        def _():
            o_ref[...] = (_dot(dg_ref[...], gates[k][...], 1, 1) + _dot(du_ref[...], ups[k][...], 1, 1)).astype(bf16)


def norm_bwd(p, dg, du, gates, ups):
    tokens, ff = dg.shape
    n = gates[0].shape[0]
    d = RUNS * n
    per = n // TILE
    starts = [0]
    for run in gates:
        starts.append(starts[-1] + run.shape[0] // TILE)
    whole = pl.BlockSpec((tokens, ff), lambda i, p: (0, 0))
    runs = [pl.BlockSpec((TILE, ff), lambda i, p, s=s, e=e: (jnp.clip(i - s, 0, e - s - 1), 0)) for s, e in zip(starts, starts[1:])]
    return _call(functools.partial(_norm_bwd, starts), p, RUNS * per, (dg, du, *gates, *ups), [whole, whole, *runs, *runs],
                 jax.ShapeDtypeStruct((tokens, d), bf16), pl.BlockSpec((tokens, TILE), lambda i, p: (0, (i // per ^ p[0]) * per + i % per)),
                 4 * tokens * d * ff)


def _by_weight(p_ref, a_near, a_far, b_near, b_far, o_ref):
    for at in range(0, o_ref.shape[1], 512):
        cols = slice(at, at + 512)
        o_ref[:, cols] = (_dot(a_near[...], b_near[:, cols], 0, 0) + _dot(a_far[...], b_far[:, cols], 0, 0)).astype(bf16)


def by_weight(p, a_near, a_far, b_near, b_far, part=None):
    tokens, rows = a_near.shape
    cols, at = (b_near.shape[1], 0) if part is None else (b_near.shape[1] // 2, part)
    tile = pl.BlockSpec((tokens, TILE), lambda i, p: (0, i))
    columns = pl.BlockSpec((tokens, cols), lambda i, p: (0, at))
    return _call(_by_weight, p, rows // TILE, (a_near, a_far, b_near, b_far),
                 [tile, tile, columns, columns], jax.ShapeDtypeStruct((rows, cols), bf16),
                 pl.BlockSpec((TILE, cols), lambda i, p: (i, 0)), 4 * tokens * rows * cols)


FLIPS = {n: [(i, i ^ n) for i in range(4)] for n in (1, 2)}


def flip(t, axis, n):
    return lax.ppermute(t, axis, FLIPS[n])


def after(t, *others):
    return lax.optimization_barrier((t, *others))[0]


def gather(w):
    half = w.shape[0] // 2
    z, y = flip(w, "dp", 1), flip(w, "dp", 2)

    def far(*before):
        first = flip(after(z, *before)[:half], "dp", 2)
        second = flip(after(y, *before)[half:], "dp", 1)
        return w, z, y, first, second

    return far


def scatter(g, p):
    n = g.shape[0] // 4
    h = n // 2
    run = lambda j, at, size: lax.dynamic_slice_in_dim(g, (p ^ j) * n + at, size, axis=0)
    by_y = flip(run(3, 0, h), "dp", 2)
    by_z = flip(run(3, h, h), "dp", 1)
    got_z = flip(jnp.concatenate([add(run(1, 0, h), by_y), run(1, h, h)]), "dp", 1)
    got_y = flip(jnp.concatenate([run(2, 0, h), add(run(2, h, h), by_z)]), "dp", 2)
    return add(run(0, 0, n), got_z, got_y)


def add(*terms):
    return sum(t.astype(f32) for t in terms).astype(bf16)


def pair(own, mate, me):
    first = (jnp.arange(2) == me % 2)[:, None, None]
    return jnp.where(first, own[None], mate[None]).reshape(-1, own.shape[1])


def spread(t, me, *before):
    other = flip(t, "tp", 2)
    mate = flip(t, "tp", 1)
    near = pair(t, mate, me)

    def far(*others):
        got = after(other, *before)
        last = flip(got, "tp", 1)
        return pair(*after((got, last), *others), me)

    return near, far


def collect(near, far, me):
    n = near.shape[0] // 2
    of = lambda t, core: lax.dynamic_slice_in_dim(t, core * n, n, axis=0)
    core = me % 2
    to_x = add(of(far, core), flip(of(far, 1 - core), "tp", 1))
    got = flip(to_x, "tp", 2)
    return add(of(near, core), flip(of(near, 1 - core), "tp", 1), got)


def dot(a, b, ca=1, cb=0):
    return _dot(a, b, ca, cb)


def mm(a, b, ca=1, cb=0):
    return dot(a, b, ca, cb).astype(bf16)


def rms(h):
    wide = h.astype(f32)
    return lax.rsqrt(jnp.mean(wide**2, -1, keepdims=True) + 1e-6)


def rms_bwd(h, scale, d):
    wide, d = h.astype(f32), d.astype(f32)
    return scale * d - wide * (scale**3 * jnp.mean(d * wide, -1, keepdims=True))


def whole(runs, p):
    n = runs[0].shape[0]
    full = jnp.zeros((4 * n, runs[0].shape[1]), runs[0].dtype)
    for j, run in enumerate(runs[:3]):
        full = lax.dynamic_update_slice_in_dim(full, run, (p ^ j) * n, axis=0)
    for i, run in enumerate(runs[3:]):
        full = lax.dynamic_update_slice_in_dim(full, run, (p ^ 3) * n + i * (n // 2), axis=0)
    return full


def solution(mesh):
    def layer(x, dy, wq, wk, wv, wo, w_gate, w_up, w_down):
        x, dy = x[0], dy[0]
        p, me = lax.axis_index("dp"), lax.axis_index("tp")
        tokens = 4 * x.shape[0]
        half = HEAD // 2
        angle = jnp.arange(tokens, dtype=f32)[:, None] * THETA ** (-jnp.arange(half, dtype=f32) / half)
        cos, sin = jnp.cos(angle), jnp.sin(angle)
        cos, sin = jnp.concatenate([cos, cos], -1), jnp.concatenate([-sin, sin], -1)
        me1 = (me // 2 * 2).astype(jnp.int32).reshape(1)

        both = lambda s, t: jnp.concatenate([s, t])
        m = x.shape[0]

        w_qkv = jnp.concatenate([wq, wk, wv], axis=1)
        w_o = whole(gather(wo)(), p)
        runs = gather(w_qkv)()
        dy_other = flip(dy, "tp", 2)
        w_qkv = whole(runs, p)
        gates, ups = gather(w_gate), gather(w_up)

        s1 = rms(x)
        a = (x.astype(f32) * s1).astype(bf16)
        a_near, a_far = spread(a, me, w_qkv, cos, sin)
        qkv_near = mm(a_near, w_qkv)
        a_far = a_far(qkv_near)
        qkv = both(qkv_near, mm(a_far, w_qkv))
        heads, lse = attend(me1, qkv, cos, sin)
        o_far = mm(heads[2 * m :], w_o)
        o_near = mm(after(heads, o_far)[: 2 * m], w_o)
        gates, ups = gates(o_near), ups(o_near)
        h = x + collect(o_near, o_far, me)
        s2 = rms(h)
        b = (h.astype(f32) * s2).astype(bf16)
        dy_near = pair(dy, flip(after(dy, o_near), "tp", 1), me)
        dy_far = pair(dy_other, flip(after(dy_other, o_near), "tp", 1), me)
        place = p.astype(jnp.int32).reshape(1)
        b_near, b_far = spread(b, me)
        w_d = lax.all_gather(after(w_down, b_near), "dp", axis=0, tiled=True)
        gate_near = gate_up(place, b_near, gates=gates)
        up_near, hid_near = gate_up(place, b_near, ups=ups, gate=gate_near)
        b_far = b_far(hid_near)
        gate_far, up_far, hid_far = gate_up(place, b_far, gates, ups)
        g_down = by_weight(place, hid_near, hid_far, dy_near, dy_far)
        dg_far, du_far = hidden_bwd(place, after(dy_far, g_down), w_d, gate_far, up_far)
        db_far = norm_bwd(place, dg_far, du_far, gates, ups)
        dg_near, du_near = hidden_bwd(place, after(dy_near, db_far), w_d, gate_near, up_near)
        g_gate = by_weight(place, b_near, b_far, dg_near, dg_far)
        db_near = norm_bwd(place, *after((dg_near, du_near), g_gate), gates, ups)
        d_b = collect(db_near, db_far, me)
        d_h = dy + rms_bwd(h, s2, d_b).astype(bf16)
        dh_near, dh_far = spread(d_h, me)
        g_up = by_weight(place, b_near, b_far, after(du_near, d_h), du_far)
        do_near = mm(after(dh_near, g_up), w_o, 1, 1)
        dh_far = dh_far(do_near)
        do = both(do_near, mm(dh_far, w_o, 1, 1))
        d_qkv = attend_bwd(me1, qkv, cos, sin, heads, do, lse)
        da_far = mm(d_qkv[2 * m :], w_qkv, 1, 1)
        g_o = mm(heads, both(dh_near, dh_far), 0, 0)
        da_near = mm(after(d_qkv, da_far)[: 2 * m], w_qkv, 1, 1)
        g_qkv = mm(both(a_near, a_far), after(d_qkv, da_near), 0, 0)
        d_a = collect(da_near, da_far, me)
        d_x = (d_h + rms_bwd(x, s1, d_a).astype(bf16))[None]

        def total(g):
            return lax.psum_scatter(g, "dp", scatter_dimension=0, tiled=True)

        r_down, r_up, r_o = total(g_down), total(g_up), scatter(g_o, p)
        r_gate = total(g_gate)
        r_qkv = scatter(g_qkv, p)
        cut = wq.shape[1]
        r_q, r_k, r_v = r_qkv[:, :cut], r_qkv[:, cut : cut + HEAD], r_qkv[:, cut + HEAD :]
        return d_x, r_q, r_k, r_v, r_o, r_gate, r_up, r_down

    states, by_columns, by_rows = P("dp", "tp", None), P("dp", "tp"), P(("tp", "dp"), None)
    weights = (by_columns, by_columns, by_columns, by_rows, by_columns, by_columns, by_rows)
    return jax.shard_map(layer, mesh=mesh, in_specs=(states, states, *weights), out_specs=(states, *weights), check_vma=False)
```
